32 devices in a mesh: blk: 16 (over z, y, core), grp: 2 (over x).
Axes of the slice: x: 2, y: 2, z: 4, core: 2. Of those that a mesh axis runs over, the one named last changes fastest.
Arguments:
- layer_one: bfloat16 [1792, 1024], P(('blk', 'grp')), may hold values from -6 to 6
- layer_two: bfloat16 [1792, 1024], P(('blk', 'grp')), may hold values from -6 to 6
- spread: int32 [2], replicated, may hold values from 1024 to 4096
Outputs:
- profiles: float32 [2, 1792], P(None, ('blk', 'grp'))
- alignment: float32 [], replicated
The draws below stay inside these ranges and needn't reach their ends.
All inputs are finite; a program needn't handle non-finite values.
Results may differ from the reference program's by a relative error of at most 0.0003.
Values may be sent and summed in bfloat16 or wider, within the bound.
A program may use at most 128 MiB of HBM per device.

```python
import jax
import jax.numpy as jnp
from jax import lax

D = 1024
ROWS_DEV = 56
N = 1792


def steps_of(own_key, extent, pieces, least, high):
    def one(axis_at, parts):
        steps = jax.random.uniform(jax.random.fold_in(jax.random.fold_in(own_key, 6), axis_at), (parts,), jnp.float32, least / len(pieces), high / len(pieces))
        return jnp.repeat(jnp.exp(steps), extent[axis_at] // parts).reshape((-1,) + (1,) * (len(extent) - axis_at - 1))

    level = one(*pieces[0])
    for cut in pieces[1:]:
        level = level * one(*cut)
    return level


def normal_values(own_key, dims, scale, bound, shards=(), kind=jnp.bfloat16):
    result = scale * jax.random.normal(own_key, dims, jnp.float32)
    if shards:
        result = result * steps_of(own_key, dims, shards, -0.22, 0.18)
    return jnp.clip(result, -bound, bound).astype(kind)


def setup_inputs(seed: int = 0) -> dict:
    streams_of = jax.random.split(jax.random.key(seed), 4)
    return {
        "layer_one": normal_values(streams_of[0], (N, D), 1.0, 6.0, ((0, 32),)),
        "layer_two": normal_values(streams_of[1], (N, D), 1.0, 6.0, ((0, 32),)),
        "spread": jax.random.randint(streams_of[2], (2,), D, 4 * D + 1).astype(jnp.int32),
    }


def reference(layer_one, layer_two, spread):
    total = layer_one.shape[0]
    block_rows = 2 * ROWS_DEV
    scales = spread.astype(jnp.float32)
    offsets = jnp.exp(-D / scales)
    sq_one = lax.optimization_barrier(jnp.sum(layer_one.astype(jnp.float32) ** 2, axis=1))
    sq_two = lax.optimization_barrier(jnp.sum(layer_two.astype(jnp.float32) ** 2, axis=1))

    def kernel(rows, sq_rows, whole, sq_whole, scale, offset):
        inner = lax.dot_general(rows, whole, (((1,), (1,)), ((), ())), preferred_element_type=jnp.float32)
        dist = sq_rows[:, None] + sq_whole[None, :] - 2.0 * inner
        return jnp.exp(-dist / (2.0 * scale)) - offset

    def one_block(index):
        start = index * block_rows
        rows_one = lax.dynamic_slice_in_dim(layer_one, start, block_rows, 0)
        rows_two = lax.dynamic_slice_in_dim(layer_two, start, block_rows, 0)
        norm_one = lax.dynamic_slice_in_dim(sq_one, start, block_rows, 0)
        norm_two = lax.dynamic_slice_in_dim(sq_two, start, block_rows, 0)
        first = kernel(rows_one, norm_one, layer_one, sq_one, scales[0], offsets[0])
        second = kernel(rows_two, norm_two, layer_two, sq_two, scales[1], offsets[1])
        return (lax.optimization_barrier(jnp.sum(first, axis=1)), lax.optimization_barrier(jnp.sum(second, axis=1)), jnp.sum(first * second), jnp.sum(first * first), jnp.sum(second * second))
    results = lax.map(one_block, jnp.arange(total // block_rows, dtype=jnp.int32))
    row_one = results[0].reshape(-1)
    row_two = results[1].reshape(-1)
    cross, self_one, self_two = (jnp.sum(results[2]), jnp.sum(results[3]), jnp.sum(results[4]))
    sum_one, sum_two = (jnp.sum(row_one), jnp.sum(row_two))
    c_cross = jnp.sum(row_one * row_two)
    c_one = jnp.sum(row_one * row_one)
    c_two = jnp.sum(row_two * row_two)
    h_cross = cross - 2.0 * c_cross / total + sum_one * sum_two / (total * total)
    h_one = self_one - 2.0 * c_one / total + sum_one * sum_one / (total * total)
    h_two = self_two - 2.0 * c_two / total + sum_two * sum_two / (total * total)
    alignment = h_cross / jnp.sqrt(h_one * h_two)
    profiles = jnp.stack([row_one / jnp.sqrt(c_one / total), row_two / jnp.sqrt(c_two / total)])
    return (profiles, alignment)
```

```python
import functools

import jax
import jax.numpy as jnp
from jax import lax
from jax.experimental import pallas as pl
from jax.experimental.pallas import tpu as pltpu
from jax.sharding import PartitionSpec as P

MESH = pl.DeviceIdType.MESH
LANES = 128
PLANE = 4


def reach(planes, src):
    if planes % 2:
        return planes // 2
    ahead = 1 - (2 * src) // planes
    odd = (src - (planes // 2) * (1 - ahead)) % 2
    return planes // 2 - 1 + ahead * (1 - odd) + (1 - ahead) * odd


def round_up(value, step):
    return -(-value // step) * step


def body(blks, grps, rows, one_ref, two_ref, spread_ref, prof_ref, align_ref, plane, column, outbox, inbox, col_out, col_in, sums, got,
         load_sem, psend, precv, csend, crecv, osend, orecv, rsend, rrecv, ssend, srecv):
    planes = blks // PLANE
    n = blks * grps
    depth = one_ref.shape[1]
    pad = plane.shape[2] // (2 * 4)
    width = plane.shape[2]
    half = depth // 2
    blk = lax.axis_index("blk")
    grp = lax.axis_index("grp")
    k = blk // PLANE
    y = (blk // 2) % 2
    core = blk % 2
    me = blk * grps + grp

    def at(plane_at, y_at, core_at, grp_at):
        return (plane_at * PLANE + y_at * 2 + core_at, grp_at)

    def place(slot, side):
        return (slot * 2 + side) * pad

    loads = []
    for layer, ref in enumerate((one_ref, two_ref)):
        copy = pltpu.make_async_copy(ref, plane.at[layer, 0, pl.ds(0, rows)], load_sem.at[layer])
        copy.start()
        loads.append(copy)

    barrier = pltpu.get_barrier_semaphore()

    def greet(off, carry):
        other = lax.rem(me + off, n)
        pl.semaphore_signal(barrier, inc=1, device_id=(other // grps, other % grps), device_id_type=MESH)
        return carry

    lax.fori_loop(1, n, greet, 0)
    for copy in loads:
        copy.wait()
    pl.semaphore_wait(barrier, n - 1)

    x_peer = at(k, y, core, 1 - grp)
    y_peer = at(k, 1 - y, core, grp)
    d_peer = at(k, 1 - y, core, 1 - grp)
    peers = (None, x_peer, y_peer, d_peer)
    mates = (at(k, y, 1 - core, grp), at(k, y, 1 - core, 1 - grp), at(k, 1 - y, 1 - core, grp), at(k, 1 - y, 1 - core, 1 - grp))

    def plane_copy(layer, src, slot, side, device):
        return pltpu.make_async_remote_copy(
            src_ref=plane.at[layer, 0, pl.ds(place(*src), rows)],
            dst_ref=plane.at[layer, 0, pl.ds(place(slot, side), rows)],
            send_sem=psend.at[slot, side, layer],
            recv_sem=precv.at[slot, side, layer],
            device_id=device,
            device_id_type=MESH,
        )

    def x_own(layer):
        return plane_copy(layer, (0, 0), 1, 0, x_peer)

    def y_own(layer):
        return plane_copy(layer, (0, 0), 2, 0, y_peer)

    def diag(layer):
        if layer == 0:
            return plane_copy(0, (1, 0), 3, 0, y_peer)
        return plane_copy(1, (2, 0), 3, 0, x_peer)

    def mate(slot, layer):
        return plane_copy(layer, (slot, 0), slot, 1, mates[0])

    def col_copy(src, way, layer, part, own, dst):
        if own:
            ref = plane.at[layer, 0, pl.ds(0, rows), pl.ds(part * half, half)]
        else:
            ref = column.at[src, layer, pl.ds(0, rows), pl.ds(part * half, half)]
        return pltpu.make_async_remote_copy(
            src_ref=ref,
            dst_ref=column.at[src, layer, pl.ds(0, rows), pl.ds(part * half, half)],
            send_sem=csend.at[src, way, layer, part],
            recv_sem=crecv.at[src, layer, part],
            device_id=at(dst, y, core, grp),
            device_id_type=MESH,
        )

    pieces = [(layer, part) for layer in range(2) for part in range(2)]

    def gets(src, dst):
        gap = (dst - src + 2 * planes) % planes
        return (src >= 0) & (src < planes) & (dst >= 0) & (dst < planes) & (gap > 0) & (gap <= reach(planes, src))

    last_down = k + reach(planes, k) - planes
    starts = ((0, k + 1, gets(k, k + 1)), (1, last_down, last_down >= 0))

    def each_source(work):
        def step(index, carry):
            way = index % 2
            src = k - (index // 2 + 1) * (1 - 2 * way)
            onward = k + 1 - 2 * way

            @pl.when(gets(src, k))
            def _():
                work(src, way, onward, gets(src, onward) & (onward != src))

            return carry

        lax.fori_loop(0, 2 * (planes - 1), step, 0)

    x_own(0).start()
    y_own(1).start()
    for way, dst, goes in starts:
        @pl.when(goes)
        def _(way=way, dst=dst):
            for layer, part in pieces:
                col_copy(k, way, layer, part, True, dst).start()
    x_own(1).start()
    y_own(0).start()
    mate(0, 0).start()
    mate(0, 1).start()

    def relay(layer):
        def work(src, way, onward, goes):
            @pl.when(goes)
            def _():
                for part in range(2):
                    col_copy(src, way, layer, part, False, onward).wait_recv()
                    col_copy(src, way, layer, part, False, onward).start()

        each_source(work)

    x_own(0).wait_recv()
    diag(0).start()
    mate(1, 0).start()
    y_own(1).wait_recv()
    diag(1).start()
    mate(2, 1).start()
    relay(0)
    x_own(1).wait_recv()
    mate(1, 1).start()
    y_own(0).wait_recv()
    mate(2, 0).start()
    relay(1)
    for layer in range(2):
        diag(layer).wait_recv()
        mate(3, layer).start()
    for slot in range(4):
        for layer in range(2):
            mate(slot, layer).wait_recv()

    scales = [jnp.full((1, 1), spread_ref[layer], jnp.int32).astype(jnp.float32) for layer in range(2)]
    rates = [-0.5 / scale for scale in scales]
    offsets = [jnp.exp(-depth / scale) for scale in scales]
    row_ok = lax.broadcasted_iota(jnp.int32, (pad, width), 0) < rows
    col_ok = lax.broadcasted_iota(jnp.int32, (pad, width), 1) % pad < rows
    ok = row_ok & col_ok

    def squares(block):
        wide = block.astype(jnp.float32)
        return jnp.sum(wide * wide, axis=1, keepdims=True)

    sq_cols = []
    for layer in range(2):
        parts = []
        for piece in range(width // LANES):
            sq = squares(plane[layer, 0, piece * LANES:(piece + 1) * LANES, :])
            parts.append(jnp.transpose(jnp.broadcast_to(sq, (LANES, LANES)))[0:1, :])
        sq_cols.append(jnp.concatenate(parts, axis=1))

    def kernel_block(layer, block):
        inner = lax.dot_general(block, plane[layer, 0], (((1,), (1,)), ((), ())), preferred_element_type=jnp.float32)
        dist = squares(block) + sq_cols[layer] - 2.0 * inner
        return jnp.where(ok, jnp.exp(dist * rates[layer]) - offsets[layer], 0.0)

    def fold(value):
        total = value[:, 0:LANES]
        for piece in range(1, width // LANES):
            total = total + value[:, piece * LANES:(piece + 1) * LANES]
        return total

    def row_sums(value):
        part = fold(value)
        if pad < LANES:
            part = jnp.concatenate([part, jnp.zeros((LANES - pad, LANES), jnp.float32)], axis=0)
        return jnp.sum(jnp.transpose(part), axis=0, keepdims=True)

    def lane_sums(value):
        return jnp.sum(fold(value), axis=0, keepdims=True)

    own = [kernel_block(layer, plane[layer, 0, 0:pad, :]) for layer in range(2)]
    sums[0:1, :] = row_sums(own[0])
    sums[1:2, :] = row_sums(own[1])
    sums[2:3, :] = lane_sums(own[0] * own[1])
    sums[3:4, :] = lane_sums(own[0] * own[0])
    sums[4:5, :] = lane_sums(own[1] * own[1])
    outbox[...] = jnp.zeros_like(outbox)
    col_out[...] = jnp.zeros_like(col_out)

    def back(src, dst):
        return pltpu.make_async_remote_copy(
            src_ref=col_out.at[src],
            dst_ref=col_in.at[dst],
            send_sem=rsend.at[src],
            recv_sem=rrecv.at[dst],
            device_id=at(src, y, core, grp),
            device_id_type=MESH,
        )

    def meet(src, way, onward, goes):
        @pl.when(jnp.logical_not(goes))
        def _():
            for layer, part in pieces:
                col_copy(src, way, layer, part, False, k).wait_recv()

        met = [kernel_block(layer, column[src, layer]) for layer in range(2)]
        for layer in range(2):
            col_out[src, layer:layer + 1, :] = row_sums(met[layer])
        back(src, k).start()
        sums[2:3, :] += 2.0 * lane_sums(met[0] * met[1])
        sums[3:4, :] += 2.0 * lane_sums(met[0] * met[0])
        sums[4:5, :] += 2.0 * lane_sums(met[1] * met[1])
        for layer in range(2):
            across = jnp.sum(met[layer], axis=0, keepdims=True)
            for place_at in range(8):
                outbox[place_at, layer:layer + 1, 0:pad] += across[:, place_at * pad:(place_at + 1) * pad]

    each_source(meet)

    def share(place_at):
        slot, side = place_at // 2, place_at % 2
        device = mates[slot] if side else peers[slot]
        return pltpu.make_async_remote_copy(
            src_ref=outbox.at[place_at],
            dst_ref=inbox.at[place_at],
            send_sem=osend.at[place_at],
            recv_sem=orecv.at[place_at],
            device_id=device,
            device_id_type=MESH,
        )

    for place_at in range(7, 0, -1):
        share(place_at).start()
    sums[0:2, :] += outbox[0, 0:2, :]
    for place_at in range(1, 8):
        share(place_at).wait_recv()
        sums[0:2, :] += inbox[place_at, 0:2, :]
    def collect(dst, carry):
        @pl.when(gets(k, dst))
        def _():
            back(k, dst).wait_recv()
            sums[0:2, :] += col_in[dst, 0:2, :]

        return carry

    lax.fori_loop(0, planes, collect, 0)

    first, second = sums[0:1, :], sums[1:2, :]
    terms = jnp.concatenate([sums[2:5, :], first, second, first * second, first * first, second * second], axis=0)
    totals = jnp.sum(terms, axis=1, keepdims=True)
    spread_out = lax.broadcasted_iota(jnp.int32, (8, LANES), 0) == lax.broadcasted_iota(jnp.int32, (8, LANES), 1)
    got[0] = jnp.sum(jnp.where(spread_out, totals, 0.0), axis=0, keepdims=True)

    def tell(off):
        other = lax.rem(me + off, n)
        return pltpu.make_async_remote_copy(
            src_ref=got.at[0],
            dst_ref=got.at[off],
            send_sem=ssend.at[off],
            recv_sem=srecv.at[off],
            device_id=(other // grps, other % grps),
            device_id_type=MESH,
        )

    def each_other(act):
        def step(off, carry):
            act(tell(off))
            return carry

        lax.fori_loop(1, n, step, 0)

    each_other(lambda copy: copy.start())

    for layer in range(2):
        x_own(layer).wait_send()
        y_own(layer).wait_send()
        diag(layer).wait_send()
        for slot in range(4):
            mate(slot, layer).wait_send()
    for way, dst, goes in starts:
        @pl.when(goes)
        def _(way=way, dst=dst):
            for layer, part in pieces:
                col_copy(k, way, layer, part, True, dst).wait_send()

    def drain(src, way, onward, goes):
        back(src, k).wait_send()

        @pl.when(goes)
        def _():
            for layer, part in pieces:
                col_copy(src, way, layer, part, False, onward).wait_send()

    each_source(drain)
    for place_at in range(1, 8):
        share(place_at).wait_send()

    each_other(lambda copy: copy.wait_recv())
    each_other(lambda copy: copy.wait_send())
    final = jnp.sum(got[...], axis=0)
    f_cross, f_one, f_two, s_one, s_two, c_cross, c_one, c_two = (final[:, at_lane:at_lane + 1] for at_lane in range(8))
    total = float(n * rows)
    h_cross = f_cross - 2.0 * c_cross / total + s_one * s_two / (total * total)
    h_one = f_one - 2.0 * c_one / total + s_one * s_one / (total * total)
    h_two = f_two - 2.0 * c_two / total + s_two * s_two / (total * total)
    align_ref[...] = h_cross / jnp.sqrt(h_one * h_two)
    prof_ref[0:1, :] = first[:, 0:rows] / jnp.sqrt(c_one / total)
    prof_ref[1:2, :] = second[:, 0:rows] / jnp.sqrt(c_two / total)


def shards(blks, grps, layer_one, layer_two, spread):
    rows, depth = layer_one.shape
    pad = round_up(rows, 64)
    planes, n = blks // PLANE, blks * grps
    dma = pltpu.SemaphoreType.DMA
    profiles, alignment = pl.pallas_call(
        functools.partial(body, blks, grps, rows),
        out_shape=(jax.ShapeDtypeStruct((2, rows), jnp.float32), jax.ShapeDtypeStruct((1, 1), jnp.float32)),
        in_specs=[pl.BlockSpec(memory_space=pl.ANY), pl.BlockSpec(memory_space=pl.ANY), pl.BlockSpec(memory_space=pltpu.SMEM)],
        out_specs=(pl.BlockSpec(memory_space=pltpu.VMEM), pl.BlockSpec(memory_space=pltpu.VMEM)),
        scratch_shapes=[
            pltpu.VMEM((2, 1, 8 * pad, depth), jnp.bfloat16),
            pltpu.VMEM((planes, 2, pad, depth), jnp.bfloat16),
            pltpu.VMEM((8, 8, LANES), jnp.float32),
            pltpu.VMEM((8, 8, LANES), jnp.float32),
            pltpu.VMEM((planes, 8, LANES), jnp.float32),
            pltpu.VMEM((planes, 8, LANES), jnp.float32),
            pltpu.VMEM((8, LANES), jnp.float32),
            pltpu.VMEM((n, 1, LANES), jnp.float32),
            dma((2,)),
            dma((4, 2, 2)),
            dma((4, 2, 2)),
            dma((planes, 2, 2, 2)),
            dma((planes, 2, 2)),
            dma((8,)),
            dma((8,)),
            dma((planes,)),
            dma((planes,)),
            dma((n,)),
            dma((n,)),
        ],
        compiler_params=pltpu.CompilerParams(collective_id=0, has_side_effects=True),
    )(layer_one, layer_two, spread)
    return (profiles, alignment.reshape(()))


def solution(mesh):
    return jax.shard_map(
        functools.partial(shards, mesh.shape["blk"], mesh.shape["grp"]),
        mesh=mesh,
        in_specs=(P(("blk", "grp"), None), P(("blk", "grp"), None), P()),
        out_specs=(P(None, ("blk", "grp")), P()),
        check_vma=False,
    )
```

```python
import functools

import jax
import jax.numpy as jnp
from jax import lax
from jax.experimental import pallas as pl
from jax.experimental.pallas import tpu as pltpu
from jax.sharding import PartitionSpec as P

MESH = pl.DeviceIdType.MESH
LANES = 128
PLANE = 4


def reach(planes, src):
    if planes % 2:
        return planes // 2
    ahead = 1 - (2 * src) // planes
    odd = (src - (planes // 2) * (1 - ahead)) % 2
    return planes // 2 - 1 + ahead * (1 - odd) + (1 - ahead) * odd


def round_up(value, step):
    return -(-value // step) * step


def body(blks, grps, rows, one_ref, two_ref, spread_ref, prof_ref, align_ref, plane, column, outbox, inbox, col_out, col_in, sums, got,
         load_sem, psend, precv, csend, crecv, osend, orecv, rsend, rrecv, ssend, srecv):
    planes = blks // PLANE
    n = blks * grps
    depth = one_ref.shape[1]
    pad = plane.shape[2] // (2 * 4)
    width = plane.shape[2]
    half = depth // 2
    blk = lax.axis_index("blk")
    grp = lax.axis_index("grp")
    k = blk // PLANE
    y = (blk // 2) % 2
    core = blk % 2
    me = blk * grps + grp

    def at(plane_at, y_at, core_at, grp_at):
        return (plane_at * PLANE + y_at * 2 + core_at, grp_at)

    def place(slot, side):
        return (slot * 2 + side) * pad

    loads = []
    for layer, ref in enumerate((one_ref, two_ref)):
        copy = pltpu.make_async_copy(ref, plane.at[layer, 0, pl.ds(0, rows)], load_sem.at[layer])
        copy.start()
        loads.append(copy)

    barrier = pltpu.get_barrier_semaphore()

    last_down = k + reach(planes, k) - planes
    x_peer = at(k, y, core, 1 - grp)
    y_peer = at(k, 1 - y, core, grp)
    for device in (x_peer, y_peer, at(k, y, 1 - core, grp)):
        pl.semaphore_signal(barrier, inc=1, device_id=device, device_id_type=MESH)

    def greet(far, count):
        linked = (far == k + 1) | (far == k - 1) | (far == last_down) | (far + reach(planes, far) - planes == k)

        @pl.when(linked)
        def _():
            pl.semaphore_signal(barrier, inc=1, device_id=at(far, y, core, grp), device_id_type=MESH)

        return count + linked.astype(jnp.int32)

    partners = lax.fori_loop(0, planes, greet, jnp.int32(3))
    for copy in loads:
        copy.wait()
    pl.semaphore_wait(barrier, partners)

    d_peer = at(k, 1 - y, core, 1 - grp)
    peers = (None, x_peer, y_peer, d_peer)
    mates = (at(k, y, 1 - core, grp), at(k, y, 1 - core, 1 - grp), at(k, 1 - y, 1 - core, grp), at(k, 1 - y, 1 - core, 1 - grp))

    def plane_copy(layer, src, slot, side, device):
        return pltpu.make_async_remote_copy(
            src_ref=plane.at[layer, 0, pl.ds(place(*src), rows)],
            dst_ref=plane.at[layer, 0, pl.ds(place(slot, side), rows)],
            send_sem=psend.at[slot, side, layer],
            recv_sem=precv.at[slot, side, layer],
            device_id=device,
            device_id_type=MESH,
        )

    def x_own(layer):
        return plane_copy(layer, (0, 0), 1, 0, x_peer)

    def y_own(layer):
        return plane_copy(layer, (0, 0), 2, 0, y_peer)

    def diag(layer):
        if layer == 0:
            return plane_copy(0, (1, 0), 3, 0, y_peer)
        return plane_copy(1, (2, 0), 3, 0, x_peer)

    def mate(slot, layer):
        return plane_copy(layer, (slot, 0), slot, 1, mates[0])

    def col_copy(src, way, layer, part, own, dst):
        if own:
            ref = plane.at[layer, 0, pl.ds(0, rows), pl.ds(part * half, half)]
        else:
            ref = column.at[src, layer, pl.ds(0, rows), pl.ds(part * half, half)]
        return pltpu.make_async_remote_copy(
            src_ref=ref,
            dst_ref=column.at[src, layer, pl.ds(0, rows), pl.ds(part * half, half)],
            send_sem=csend.at[src, way, layer, part],
            recv_sem=crecv.at[src, layer, part],
            device_id=at(dst, y, core, grp),
            device_id_type=MESH,
        )

    pieces = [(layer, part) for layer in range(2) for part in range(2)]

    def gets(src, dst):
        gap = (dst - src + 2 * planes) % planes
        return (src >= 0) & (src < planes) & (dst >= 0) & (dst < planes) & (gap > 0) & (gap <= reach(planes, src))

    starts = ((0, k + 1, gets(k, k + 1)), (1, last_down, last_down >= 0))

    def each_source(work):
        def step(index, carry):
            way = index % 2
            src = k - (index // 2 + 1) * (1 - 2 * way)
            onward = k + 1 - 2 * way

            @pl.when(gets(src, k))
            def _():
                work(src, way, onward, gets(src, onward) & (onward != src))

            return carry

        lax.fori_loop(0, 2 * (planes - 1), step, 0)

    x_own(0).start()
    y_own(1).start()
    for way, dst, goes in starts:
        @pl.when(goes)
        def _(way=way, dst=dst):
            for layer, part in pieces:
                col_copy(k, way, layer, part, True, dst).start()
    x_own(1).start()
    y_own(0).start()
    mate(0, 0).start()
    mate(0, 1).start()

    def relay(layer):
        def work(src, way, onward, goes):
            @pl.when(goes)
            def _():
                for part in range(2):
                    col_copy(src, way, layer, part, False, onward).wait_recv()
                    col_copy(src, way, layer, part, False, onward).start()

        each_source(work)

    x_own(0).wait_recv()
    diag(0).start()
    mate(1, 0).start()
    y_own(1).wait_recv()
    diag(1).start()
    mate(2, 1).start()
    relay(0)
    x_own(1).wait_recv()
    mate(1, 1).start()
    y_own(0).wait_recv()
    mate(2, 0).start()
    relay(1)
    for layer in range(2):
        diag(layer).wait_recv()
        mate(3, layer).start()
    for slot in range(4):
        for layer in range(2):
            mate(slot, layer).wait_recv()

    scales = [jnp.full((1, 1), spread_ref[layer], jnp.int32).astype(jnp.float32) for layer in range(2)]
    rates = [-0.5 / scale for scale in scales]
    offsets = [jnp.exp(-depth / scale) for scale in scales]
    row_ok = lax.broadcasted_iota(jnp.int32, (pad, width), 0) < rows
    col_ok = lax.broadcasted_iota(jnp.int32, (pad, width), 1) % pad < rows
    ok = row_ok & col_ok

    def squares(block):
        wide = block.astype(jnp.float32)
        return jnp.sum(wide * wide, axis=1, keepdims=True)

    sq_cols = []
    for layer in range(2):
        parts = []
        for piece in range(width // LANES):
            sq = squares(plane[layer, 0, piece * LANES:(piece + 1) * LANES, :])
            parts.append(jnp.transpose(jnp.broadcast_to(sq, (LANES, LANES)))[0:1, :])
        sq_cols.append(jnp.concatenate(parts, axis=1))

    def kernel_block(layer, block):
        inner = lax.dot_general(block, plane[layer, 0], (((1,), (1,)), ((), ())), preferred_element_type=jnp.float32)
        dist = squares(block) + sq_cols[layer] - 2.0 * inner
        return jnp.where(ok, jnp.exp(dist * rates[layer]) - offsets[layer], 0.0)

    def fold(value):
        total = value[:, 0:LANES]
        for piece in range(1, width // LANES):
            total = total + value[:, piece * LANES:(piece + 1) * LANES]
        return total

    def row_sums(value):
        part = fold(value)
        if pad < LANES:
            part = jnp.concatenate([part, jnp.zeros((LANES - pad, LANES), jnp.float32)], axis=0)
        return jnp.sum(jnp.transpose(part), axis=0, keepdims=True)

    def lane_sums(value):
        return jnp.sum(fold(value), axis=0, keepdims=True)

    own = [kernel_block(layer, plane[layer, 0, 0:pad, :]) for layer in range(2)]
    sums[0:1, :] = row_sums(own[0])
    sums[1:2, :] = row_sums(own[1])
    sums[2:3, :] = lane_sums(own[0] * own[1])
    sums[3:4, :] = lane_sums(own[0] * own[0])
    sums[4:5, :] = lane_sums(own[1] * own[1])
    outbox[...] = jnp.zeros_like(outbox)
    col_out[...] = jnp.zeros_like(col_out)

    def back(src, dst):
        return pltpu.make_async_remote_copy(
            src_ref=col_out.at[src],
            dst_ref=col_in.at[dst],
            send_sem=rsend.at[src],
            recv_sem=rrecv.at[dst],
            device_id=at(src, y, core, grp),
            device_id_type=MESH,
        )

    def meet(src, way, onward, goes):
        @pl.when(jnp.logical_not(goes))
        def _():
            for layer, part in pieces:
                col_copy(src, way, layer, part, False, k).wait_recv()

        met = [kernel_block(layer, column[src, layer]) for layer in range(2)]
        for layer in range(2):
            col_out[src, layer:layer + 1, :] = row_sums(met[layer])
        back(src, k).start()
        sums[2:3, :] += 2.0 * lane_sums(met[0] * met[1])
        sums[3:4, :] += 2.0 * lane_sums(met[0] * met[0])
        sums[4:5, :] += 2.0 * lane_sums(met[1] * met[1])
        for layer in range(2):
            across = jnp.sum(met[layer], axis=0, keepdims=True)
            for place_at in range(8):
                outbox[place_at, layer:layer + 1, 0:pad] += across[:, place_at * pad:(place_at + 1) * pad]

    each_source(meet)

    def share(place_at):
        slot, side = place_at // 2, place_at % 2
        device = mates[slot] if side else peers[slot]
        return pltpu.make_async_remote_copy(
            src_ref=outbox.at[place_at],
            dst_ref=inbox.at[place_at],
            send_sem=osend.at[0],
            recv_sem=orecv.at[0],
            device_id=device,
            device_id_type=MESH,
        )

    for place_at in range(7, 0, -1):
        share(place_at).start()
    sums[0:2, :] += outbox[0, 0:2, :]
    shared = inbox.at[pl.ds(1, 7)]
    pltpu.make_async_copy(shared, shared, orecv.at[0]).wait()
    sums[0:2, :] += jnp.sum(inbox[1:8], axis=0)
    def collect(dst, carry):
        @pl.when(gets(k, dst))
        def _():
            back(k, dst).wait_recv()
            sums[0:2, :] += col_in[dst, 0:2, :]

        return carry

    lax.fori_loop(0, planes, collect, 0)

    first, second = sums[0:1, :], sums[1:2, :]
    terms = jnp.concatenate([sums[2:5, :], first, second, first * second, first * first, second * second], axis=0)
    totals = jnp.sum(terms, axis=1, keepdims=True)
    spread_out = lax.broadcasted_iota(jnp.int32, (8, LANES), 0) == lax.broadcasted_iota(jnp.int32, (8, LANES), 1)
    got[0] = jnp.sum(jnp.where(spread_out, totals, 0.0), axis=0, keepdims=True)

    def tell(off):
        other = lax.rem(me + off, n)
        return pltpu.make_async_remote_copy(
            src_ref=got.at[0],
            dst_ref=got.at[off],
            send_sem=ssend.at[0],
            recv_sem=srecv.at[0],
            device_id=(other // grps, other % grps),
            device_id_type=MESH,
        )

    def start_tell(off, carry):
        tell(off).start()
        return carry

    lax.fori_loop(1, n, start_tell, 0, unroll=n <= 64)

    for layer in range(2):
        x_own(layer).wait_send()
        y_own(layer).wait_send()
        diag(layer).wait_send()
        for slot in range(4):
            mate(slot, layer).wait_send()
    for way, dst, goes in starts:
        @pl.when(goes)
        def _(way=way, dst=dst):
            for layer, part in pieces:
                col_copy(k, way, layer, part, True, dst).wait_send()

    def drain(src, way, onward, goes):
        back(src, k).wait_send()

        @pl.when(goes)
        def _():
            for layer, part in pieces:
                col_copy(src, way, layer, part, False, onward).wait_send()

    each_source(drain)
    pltpu.make_async_copy(shared, shared, osend.at[0]).wait()

    all_told = got.at[pl.ds(1, n - 1)]
    pltpu.make_async_copy(all_told, all_told, srecv.at[0]).wait()
    pltpu.make_async_copy(all_told, all_told, ssend.at[0]).wait()
    final = jnp.sum(got[...], axis=0)
    f_cross, f_one, f_two, s_one, s_two, c_cross, c_one, c_two = (final[:, at_lane:at_lane + 1] for at_lane in range(8))
    total = float(n * rows)
    h_cross = f_cross - 2.0 * c_cross / total + s_one * s_two / (total * total)
    h_one = f_one - 2.0 * c_one / total + s_one * s_one / (total * total)
    h_two = f_two - 2.0 * c_two / total + s_two * s_two / (total * total)
    align_ref[...] = h_cross / jnp.sqrt(h_one * h_two)
    prof_ref[0:1, :] = first[:, 0:rows] / jnp.sqrt(c_one / total)
    prof_ref[1:2, :] = second[:, 0:rows] / jnp.sqrt(c_two / total)


def shards(blks, grps, layer_one, layer_two, spread):
    rows, depth = layer_one.shape
    pad = round_up(rows, 64)
    planes, n = blks // PLANE, blks * grps
    dma = pltpu.SemaphoreType.DMA
    profiles, alignment = pl.pallas_call(
        functools.partial(body, blks, grps, rows),
        out_shape=(jax.ShapeDtypeStruct((2, rows), jnp.float32), jax.ShapeDtypeStruct((1, 1), jnp.float32)),
        in_specs=[pl.BlockSpec(memory_space=pl.ANY), pl.BlockSpec(memory_space=pl.ANY), pl.BlockSpec(memory_space=pltpu.SMEM)],
        out_specs=(pl.BlockSpec(memory_space=pltpu.VMEM), pl.BlockSpec(memory_space=pltpu.VMEM)),
        scratch_shapes=[
            pltpu.VMEM((2, 1, 8 * pad, depth), jnp.bfloat16),
            pltpu.VMEM((planes, 2, pad, depth), jnp.bfloat16),
            pltpu.VMEM((8, 2, LANES), jnp.float32),
            pltpu.VMEM((8, 2, LANES), jnp.float32),
            pltpu.VMEM((planes, 2, LANES), jnp.float32),
            pltpu.VMEM((planes, 2, LANES), jnp.float32),
            pltpu.VMEM((8, LANES), jnp.float32),
            pltpu.VMEM((n, 1, LANES), jnp.float32),
            dma((2,)),
            dma((4, 2, 2)),
            dma((4, 2, 2)),
            dma((planes, 2, 2, 2)),
            dma((planes, 2, 2)),
            dma((8,)),
            dma((8,)),
            dma((planes,)),
            dma((planes,)),
            dma((n,)),
            dma((n,)),
        ],
        compiler_params=pltpu.CompilerParams(collective_id=0, has_side_effects=True),
    )(layer_one, layer_two, spread)
    return (profiles, alignment.reshape(()))


def solution(mesh):
    return jax.shard_map(
        functools.partial(shards, mesh.shape["blk"], mesh.shape["grp"]),
        mesh=mesh,
        in_specs=(P(("blk", "grp"), None), P(("blk", "grp"), None), P()),
        out_specs=(P(None, ("blk", "grp")), P()),
        check_vma=False,
    )
```

```python
import functools

import jax
import jax.numpy as jnp
from jax import lax
from jax.experimental import pallas as pl
from jax.experimental.pallas import tpu as pltpu
from jax.sharding import PartitionSpec as P

MESH = pl.DeviceIdType.MESH
LANES = 128
PLANE = 4


def reach(planes, src):
    if planes % 2:
        return planes // 2
    ahead = 1 - (2 * src) // planes
    odd = (src - (planes // 2) * (1 - ahead)) % 2
    return planes // 2 - 1 + ahead * (1 - odd) + (1 - ahead) * odd


def round_up(value, step):
    return -(-value // step) * step


def body(blks, grps, rows, one_ref, two_ref, spread_ref, prof_ref, align_ref, plane, column, outbox, inbox, col_out, col_in, sums, got,
         load_sem, psend, precv, csend, crecv, osend, orecv, rsend, rrecv, ssend, srecv):
    planes = blks // PLANE
    n = blks * grps
    depth = one_ref.shape[1]
    pad = plane.shape[2] // (2 * 4)
    width = plane.shape[2]
    half = depth // 2
    blk = lax.axis_index("blk")
    grp = lax.axis_index("grp")
    k = blk // PLANE
    y = (blk // 2) % 2
    core = blk % 2
    me = blk * grps + grp

    def at(plane_at, y_at, core_at, grp_at):
        return (plane_at * PLANE + y_at * 2 + core_at, grp_at)

    def place(slot, side):
        return (slot * 2 + side) * pad

    loads = []
    for layer, ref in enumerate((one_ref, two_ref)):
        copy = pltpu.make_async_copy(ref, plane.at[layer, 0, pl.ds(0, rows)], load_sem.at[layer])
        copy.start()
        loads.append(copy)

    barrier = pltpu.get_barrier_semaphore()

    last_down = k + reach(planes, k) - planes
    x_peer = at(k, y, core, 1 - grp)
    y_peer = at(k, 1 - y, core, grp)
    for device in (x_peer, y_peer, at(k, y, 1 - core, grp)):
        pl.semaphore_signal(barrier, inc=1, device_id=device, device_id_type=MESH)

    def greet(far, count):
        linked = (far == k + 1) | (far == k - 1) | (far == last_down) | (far + reach(planes, far) - planes == k)

        @pl.when(linked)
        def _():
            pl.semaphore_signal(barrier, inc=1, device_id=at(far, y, core, grp), device_id_type=MESH)

        return count + linked.astype(jnp.int32)

    partners = lax.fori_loop(0, planes, greet, jnp.int32(3))
    for copy in loads:
        copy.wait()
    pl.semaphore_wait(barrier, partners)

    d_peer = at(k, 1 - y, core, 1 - grp)
    peers = (None, x_peer, y_peer, d_peer)
    mates = (at(k, y, 1 - core, grp), at(k, y, 1 - core, 1 - grp), at(k, 1 - y, 1 - core, grp), at(k, 1 - y, 1 - core, 1 - grp))

    def plane_copy(layer, src, slot, side, device):
        return pltpu.make_async_remote_copy(
            src_ref=plane.at[layer, 0, pl.ds(place(*src), rows)],
            dst_ref=plane.at[layer, 0, pl.ds(place(slot, side), rows)],
            send_sem=psend.at[slot, side, layer],
            recv_sem=precv.at[slot, side, layer],
            device_id=device,
            device_id_type=MESH,
        )

    def x_own(layer):
        return plane_copy(layer, (0, 0), 1, 0, x_peer)

    def y_own(layer):
        return plane_copy(layer, (0, 0), 2, 0, y_peer)

    def diag(layer):
        if layer == 0:
            return plane_copy(0, (1, 0), 3, 0, y_peer)
        return plane_copy(1, (2, 0), 3, 0, x_peer)

    def mate(slot, layer):
        return plane_copy(layer, (slot, 0), slot, 1, mates[0])

    def col_copy(src, way, layer, part, own, dst):
        if own:
            ref = plane.at[layer, 0, pl.ds(0, rows), pl.ds(part * half, half)]
        else:
            ref = column.at[src, layer, pl.ds(0, rows), pl.ds(part * half, half)]
        return pltpu.make_async_remote_copy(
            src_ref=ref,
            dst_ref=column.at[src, layer, pl.ds(0, rows), pl.ds(part * half, half)],
            send_sem=csend.at[src, way, layer, part],
            recv_sem=crecv.at[src, layer, part],
            device_id=at(dst, y, core, grp),
            device_id_type=MESH,
        )

    pieces = [(layer, part) for layer in range(2) for part in range(2)]

    def gets(src, dst):
        gap = (dst - src + 2 * planes) % planes
        return (src >= 0) & (src < planes) & (dst >= 0) & (dst < planes) & (gap > 0) & (gap <= reach(planes, src))

    starts = ((0, k + 1, gets(k, k + 1)), (1, last_down, last_down >= 0))

    def each_source(work):
        def step(index, carry):
            way = index % 2
            src = k - (index // 2 + 1) * (1 - 2 * way)
            onward = k + 1 - 2 * way

            @pl.when(gets(src, k))
            def _():
                work(src, way, onward, gets(src, onward) & (onward != src))

            return carry

        lax.fori_loop(0, 2 * (planes - 1), step, 0)

    x_own(0).start()
    y_own(1).start()
    for way, dst, goes in starts:
        @pl.when(goes)
        def _(way=way, dst=dst):
            for layer, part in pieces:
                col_copy(k, way, layer, part, True, dst).start()
    x_own(1).start()
    y_own(0).start()
    mate(0, 0).start()
    mate(0, 1).start()

    def relay(layer):
        def work(src, way, onward, goes):
            @pl.when(goes)
            def _():
                for part in range(2):
                    col_copy(src, way, layer, part, False, onward).wait_recv()
                    col_copy(src, way, layer, part, False, onward).start()

        each_source(work)

    x_own(0).wait_recv()
    diag(0).start()
    mate(1, 0).start()
    y_own(1).wait_recv()
    diag(1).start()
    mate(2, 1).start()
    relay(0)
    x_own(1).wait_recv()
    mate(1, 1).start()
    y_own(0).wait_recv()
    mate(2, 0).start()
    relay(1)
    for layer in range(2):
        diag(layer).wait_recv()
        mate(3, layer).start()
    for slot in range(4):
        for layer in range(2):
            mate(slot, layer).wait_recv()

    scales = [jnp.full((1, 1), spread_ref[layer], jnp.int32).astype(jnp.float32) for layer in range(2)]
    rates = [-0.5 / scale for scale in scales]
    offsets = [jnp.exp(-depth / scale) for scale in scales]
    row_ok = lax.broadcasted_iota(jnp.int32, (pad, width), 0) < rows
    col_ok = lax.broadcasted_iota(jnp.int32, (pad, width), 1) % pad < rows
    ok = row_ok & col_ok

    def squares(block):
        wide = block.astype(jnp.float32)
        return jnp.sum(wide * wide, axis=1, keepdims=True)

    sq_cols = []
    for layer in range(2):
        parts = []
        for piece in range(width // LANES):
            sq = squares(plane[layer, 0, piece * LANES:(piece + 1) * LANES, :])
            parts.append(jnp.transpose(jnp.broadcast_to(sq, (LANES, LANES)))[0:1, :])
        sq_cols.append(jnp.concatenate(parts, axis=1))

    def kernel_block(layer, block):
        inner = lax.dot_general(block, plane[layer, 0], (((1,), (1,)), ((), ())), preferred_element_type=jnp.float32)
        dist = squares(block) + sq_cols[layer] - 2.0 * inner
        return jnp.where(ok, jnp.exp(dist * rates[layer]) - offsets[layer], 0.0)

    def fold(value):
        total = value[:, 0:LANES]
        for piece in range(1, width // LANES):
            total = total + value[:, piece * LANES:(piece + 1) * LANES]
        return total

    def row_sums(value):
        part = fold(value)
        if pad < LANES:
            part = jnp.concatenate([part, jnp.zeros((LANES - pad, LANES), jnp.float32)], axis=0)
        return jnp.sum(jnp.transpose(part), axis=0, keepdims=True)

    def lane_sums(value):
        return jnp.sum(fold(value), axis=0, keepdims=True)

    own = [kernel_block(layer, plane[layer, 0, 0:pad, :]) for layer in range(2)]
    sums[0:1, :] = row_sums(own[0])
    sums[1:2, :] = row_sums(own[1])
    sums[2:3, :] = lane_sums(own[0] * own[1])
    sums[3:4, :] = lane_sums(own[0] * own[0])
    sums[4:5, :] = lane_sums(own[1] * own[1])
    outbox[...] = jnp.zeros_like(outbox)
    col_out[...] = jnp.zeros_like(col_out)

    def back(src, dst):
        return pltpu.make_async_remote_copy(
            src_ref=col_out.at[src],
            dst_ref=col_in.at[dst],
            send_sem=rsend.at[src],
            recv_sem=rrecv.at[dst],
            device_id=at(src, y, core, grp),
            device_id_type=MESH,
        )

    def meet(src, way, onward, goes):
        @pl.when(jnp.logical_not(goes))
        def _():
            for layer, part in pieces:
                col_copy(src, way, layer, part, False, k).wait_recv()

        met = [kernel_block(layer, column[src, layer]) for layer in range(2)]
        for layer in range(2):
            col_out[src, layer:layer + 1, :] = row_sums(met[layer])
        back(src, k).start()
        sums[2:3, :] += 2.0 * lane_sums(met[0] * met[1])
        sums[3:4, :] += 2.0 * lane_sums(met[0] * met[0])
        sums[4:5, :] += 2.0 * lane_sums(met[1] * met[1])
        for layer in range(2):
            across = jnp.sum(met[layer], axis=0, keepdims=True)
            for place_at in range(8):
                outbox[place_at, layer:layer + 1, 0:pad] += across[:, place_at * pad:(place_at + 1) * pad]

    each_source(meet)

    def share(place_at):
        slot, side = place_at // 2, place_at % 2
        device = mates[slot] if side else peers[slot]
        return pltpu.make_async_remote_copy(
            src_ref=outbox.at[place_at],
            dst_ref=inbox.at[place_at],
            send_sem=osend.at[0],
            recv_sem=orecv.at[0],
            device_id=device,
            device_id_type=MESH,
        )

    for place_at in range(7, 0, -1):
        share(place_at).start()
    sums[0:2, :] += outbox[0, 0:2, :]
    shared = inbox.at[pl.ds(1, 7)]
    pltpu.make_async_copy(shared, shared, orecv.at[0]).wait()
    sums[0:2, :] += jnp.sum(inbox[1:8], axis=0)
    def collect(dst, carry):
        @pl.when(gets(k, dst))
        def _():
            back(k, dst).wait_recv()
            sums[0:2, :] += col_in[dst, 0:2, :]

        return carry

    lax.fori_loop(0, planes, collect, 0)

    first, second = sums[0:1, :], sums[1:2, :]
    terms = jnp.concatenate([sums[2:5, :], first, second, first * second, first * first, second * second], axis=0)
    totals = jnp.sum(terms, axis=1, keepdims=True)
    spread_out = lax.broadcasted_iota(jnp.int32, (8, LANES), 0) == lax.broadcasted_iota(jnp.int32, (8, LANES), 1)
    got[0] = jnp.sum(jnp.where(spread_out, totals, 0.0), axis=0, keepdims=True)

    def tell(off):
        other = lax.rem(me + off, n)
        return pltpu.make_async_remote_copy(
            src_ref=got.at[0],
            dst_ref=got.at[off],
            send_sem=ssend.at[0],
            recv_sem=srecv.at[0],
            device_id=(other // grps, other % grps),
            device_id_type=MESH,
        )

    def start_tell(off, carry):
        tell(off).start()
        return carry

    lax.fori_loop(1, n, start_tell, 0, unroll=n <= 64)

    for layer in range(2):
        x_own(layer).wait_send()
        y_own(layer).wait_send()
        diag(layer).wait_send()
        for slot in range(4):
            mate(slot, layer).wait_send()
    for way, dst, goes in starts:
        @pl.when(goes)
        def _(way=way, dst=dst):
            for layer, part in pieces:
                col_copy(k, way, layer, part, True, dst).wait_send()

    def drain(src, way, onward, goes):
        back(src, k).wait_send()

        @pl.when(goes)
        def _():
            for layer, part in pieces:
                col_copy(src, way, layer, part, False, onward).wait_send()

    each_source(drain)
    pltpu.make_async_copy(shared, shared, osend.at[0]).wait()

    all_told = got.at[pl.ds(1, n - 1)]
    pltpu.make_async_copy(all_told, all_told, srecv.at[0]).wait()
    pltpu.make_async_copy(all_told, all_told, ssend.at[0]).wait()
    final = jnp.sum(got[...], axis=0)
    f_cross, f_one, f_two, s_one, s_two, c_cross, c_one, c_two = (final[:, at_lane:at_lane + 1] for at_lane in range(8))
    total = float(n * rows)
    h_cross = f_cross - 2.0 * c_cross / total + s_one * s_two / (total * total)
    h_one = f_one - 2.0 * c_one / total + s_one * s_one / (total * total)
    h_two = f_two - 2.0 * c_two / total + s_two * s_two / (total * total)
    align_ref[...] = h_cross / jnp.sqrt(h_one * h_two)
    prof_ref[0:1, :] = first[:, 0:rows] / jnp.sqrt(c_one / total)
    prof_ref[1:2, :] = second[:, 0:rows] / jnp.sqrt(c_two / total)


def shards(blks, grps, layer_one, layer_two, spread):
    rows, depth = layer_one.shape
    pad = round_up(rows, 64)
    planes, n = blks // PLANE, blks * grps
    dma = pltpu.SemaphoreType.DMA
    profiles, alignment = pl.pallas_call(
        functools.partial(body, blks, grps, rows),
        out_shape=(pltpu.VMEM((2, rows), jnp.float32), pltpu.VMEM((1, 1), jnp.float32)),
        in_specs=[pl.BlockSpec(memory_space=pl.ANY), pl.BlockSpec(memory_space=pl.ANY), pl.BlockSpec(memory_space=pltpu.SMEM)],
        out_specs=(pl.BlockSpec(memory_space=pltpu.VMEM), pl.BlockSpec(memory_space=pltpu.VMEM)),
        scratch_shapes=[
            pltpu.VMEM((2, 1, 8 * pad, depth), jnp.bfloat16),
            pltpu.VMEM((planes, 2, pad, depth), jnp.bfloat16),
            pltpu.VMEM((8, 2, LANES), jnp.float32),
            pltpu.VMEM((8, 2, LANES), jnp.float32),
            pltpu.VMEM((planes, 2, LANES), jnp.float32),
            pltpu.VMEM((planes, 2, LANES), jnp.float32),
            pltpu.VMEM((8, LANES), jnp.float32),
            pltpu.VMEM((n, 1, LANES), jnp.float32),
            dma((2,)),
            dma((4, 2, 2)),
            dma((4, 2, 2)),
            dma((planes, 2, 2, 2)),
            dma((planes, 2, 2)),
            dma((8,)),
            dma((8,)),
            dma((planes,)),
            dma((planes,)),
            dma((n,)),
            dma((n,)),
        ],
        compiler_params=pltpu.CompilerParams(collective_id=0, has_side_effects=True),
    )(layer_one, layer_two, spread)
    return (profiles, alignment.reshape(()))


def solution(mesh):
    return jax.shard_map(
        functools.partial(shards, mesh.shape["blk"], mesh.shape["grp"]),
        mesh=mesh,
        in_specs=(P(("blk", "grp"), None), P(("blk", "grp"), None), P()),
        out_specs=(P(None, ("blk", "grp")), P()),
        check_vma=False,
    )
```
